32 devices in a mesh: fsdp: 16 (over z, y, core), grp: 2 (over x).
Axes of the slice: x: 2, y: 2, z: 4, core: 2. Of those that a mesh axis runs over, the one named last changes fastest.
Arguments:
- hidden: bfloat16 [8192, 3072], P('fsdp', 'grp'), may hold values from -16 to 16
- queries: bfloat16 [8192, 1536], P('fsdp', 'grp'), may hold values from -6 to 6
- attn_keys: bfloat16 [8192, 1536], P('fsdp', 'grp'), may hold values from -6 to 6
- w_value: bfloat16 [1536, 3072], P('fsdp', 'grp'), may hold values from -1 to 1
- w_out: bfloat16 [1536, 3072], P('fsdp', 'grp'), may hold values from -1 to 1
- alpha: float32 [3072], P('grp'), may hold values from 0.05 to 0.5
- out_grad: bfloat16 [8192, 3072], P('fsdp', 'grp'), may hold values from -6 to 6
Outputs:
- new_hidden: bfloat16 [8192, 3072], P('fsdp', 'grp')
- grad_hidden: bfloat16 [8192, 3072], P('fsdp', 'grp')
- grad_queries: bfloat16 [8192, 1536], P('fsdp', 'grp')
- grad_keys: bfloat16 [8192, 1536], P('fsdp', 'grp')
- grad_w_value: float32 [1536, 3072], P('fsdp', 'grp')
- grad_w_out: float32 [1536, 3072], P('fsdp', 'grp')
The draws below stay inside these ranges and needn't reach their ends.
All inputs are finite; a program needn't handle non-finite values.
Results may differ from the reference program's by a relative error of at most 0.012.
The reference program's roundings to bfloat16 on the way count: a program that leaves them out, or rounds other values in their place, can miss the bound.
Values may be sent and summed in bfloat16 or wider, within the bound.
A program may use at most 192 MiB of HBM per device.

```python
import math
import jax
import jax.numpy as jnp
from jax import lax

D = 3072
HEADS = 12
HS = 128
SEQ = 512
HD = 1536
TOKENS = 8192


def column_scales(scale_key, width):
    position = jnp.arange(width, dtype=jnp.float32) / (width - 1)
    ramp_scale = jnp.exp(jnp.log(3.0) * (position - 0.5))
    roughness = jnp.exp(jax.random.uniform(scale_key, (width,), jnp.float32, -1.0, 1.0))
    return ramp_scale * roughness


def draw_hidden(key, part):
    row_key, col_key, val_key = jax.random.split(jax.random.fold_in(key, 5), 3)
    row_scale = jnp.exp(jax.random.uniform(row_key, (TOKENS, 1), jnp.float32, -1.15, 1.15))
    col_scale = column_scales(col_key, D)
    base_draw = jax.random.normal(val_key, (TOKENS, D), jnp.float32)
    return jnp.clip(base_draw * row_scale * col_scale, -16.0, 16.0).astype(jnp.bfloat16)


def weight_rows(key):
    row_key, col_key, val_key = jax.random.split(key, 3)
    row_scale = jnp.exp(jax.random.uniform(row_key, (HD, 1), jnp.float32, 0.0, jnp.log(10.0)))
    col_scale = column_scales(col_key, D)
    base_draw = jax.random.normal(val_key, (HD, D), jnp.float32)
    scaled = base_draw * row_scale * col_scale / (10.0 * D ** 0.5)
    return jnp.clip(scaled, -1.0, 1.0).astype(jnp.bfloat16)


def draw_w_value(key, part):
    return weight_rows(jax.random.fold_in(key, 11))


def draw_w_out(key, part):
    return weight_rows(jax.random.fold_in(key, 23))


def attention_pair(key):
    query_key, keys_key = jax.random.split(jax.random.fold_in(key, 37), 2)
    query_draw = jnp.clip(jax.random.normal(query_key, (TOKENS, HD), jnp.float32), -6.0, 6.0)
    keys_draw = jnp.clip(jax.random.normal(keys_key, (TOKENS, HD), jnp.float32), -6.0, 6.0)
    return (query_draw, keys_draw)


def draw_queries(key, part):
    return attention_pair(key)[0].astype(jnp.bfloat16)


def draw_attn_keys(key, part):
    return attention_pair(key)[1].astype(jnp.bfloat16)


def levels(own_key, shape, cuts, low, high):
    def one(dim, blocks):
        draws = jax.random.uniform(jax.random.fold_in(jax.random.fold_in(own_key, 6), dim), (blocks,), jnp.float32, low / len(cuts), high / len(cuts))
        return jnp.repeat(jnp.exp(draws), shape[dim] // blocks).reshape((-1,) + (1,) * (len(shape) - dim - 1))

    gain = one(*cuts[0])
    for cut in cuts[1:]:
        gain = gain * one(*cut)
    return gain


def gaussian(key, shape, scale, limit, shards=(), kind=jnp.bfloat16):
    loudness = levels(key, shape, shards, -0.22, 0.18) if shards else 1.0
    values = jax.random.normal(key, shape, jnp.float32) * scale * loudness
    return jnp.minimum(jnp.maximum(values, -limit), limit).astype(kind)


def setup_inputs(seed: int = 0) -> dict:
    seeds = jax.random.split(jax.random.key(seed), 8)
    hidden = draw_hidden(jax.random.fold_in(seeds[7], 71), 0)
    queries = draw_queries(jax.random.fold_in(seeds[7], 71), 0)
    attn_keys = draw_attn_keys(jax.random.fold_in(seeds[7], 71), 0)
    w_value = draw_w_value(jax.random.fold_in(seeds[7], 71), 0)
    w_out = draw_w_out(jax.random.fold_in(seeds[7], 71), 0)
    alpha = jnp.clip(jnp.exp(math.log(0.5) - 2.3025851 * jax.random.uniform(seeds[5], (D,), jnp.float32) ** levels(seeds[5], (D,), ((0, 2),), -0.2, 0.2)), 0.05, 0.5)
    out_grad = gaussian(seeds[6], (TOKENS, D), 1.0, 6.0, ((0, 16), (1, 2)))
    return dict(hidden=hidden, queries=queries, attn_keys=attn_keys, w_value=w_value, w_out=w_out, alpha=alpha, out_grad=out_grad)


EPS = 1e-06

def contract_last(left, right):
    return lax.dot_general(left, right, (((1,), (1,)), ((), ())), preferred_element_type=jnp.float32)

def contract_first(left, right):
    return lax.dot_general(left, right, (((0,), (0,)), ((), ())), preferred_element_type=jnp.float32)

def causal_probs(query_head, key_head):
    length = query_head.shape[0]
    score_scale = query_head.shape[1] ** (-0.5)
    scores = contract_last(query_head, key_head) * score_scale
    row_pos = lax.broadcasted_iota(jnp.int32, (length, length), 0)
    col_pos = lax.broadcasted_iota(jnp.int32, (length, length), 1)
    scores = jnp.where(row_pos >= col_pos, scores, -1e+30)
    row_peak = lax.optimization_barrier(jnp.max(scores, axis=1, keepdims=True))
    exp_terms = jnp.exp(scores - row_peak)
    return exp_terms / lax.optimization_barrier(jnp.sum(exp_terms, axis=1, keepdims=True))

def head_forward(items):
    query_head, key_head, value_head = items
    attn_prob = causal_probs(query_head, key_head)
    return jnp.dot(attn_prob.astype(jnp.bfloat16), value_head, preferred_element_type=jnp.float32).astype(jnp.bfloat16)

def head_backward(items):
    query_head, key_head, value_head, grad_head = items
    score_scale = query_head.shape[1] ** (-0.5)
    attn_prob = causal_probs(query_head, key_head)
    prob_half = attn_prob.astype(jnp.bfloat16)
    grad_prob = contract_last(grad_head, value_head)
    row_delta = lax.optimization_barrier(jnp.sum(attn_prob * grad_prob, axis=1, keepdims=True))
    grad_score = (attn_prob * (grad_prob - row_delta)).astype(jnp.bfloat16)
    grad_query = (jnp.dot(grad_score, key_head, preferred_element_type=jnp.float32) * score_scale).astype(jnp.bfloat16)
    grad_key = (contract_first(grad_score, query_head) * score_scale).astype(jnp.bfloat16)
    grad_value = contract_first(prob_half, grad_head).astype(jnp.bfloat16)
    return (grad_query, grad_key, grad_value)

def to_heads(block):
    return block.reshape(TOKENS // SEQ, SEQ, HEADS, HS).transpose(0, 2, 1, 3).reshape(-1, SEQ, HS)

def from_heads(stacked):
    return stacked.reshape(TOKENS // SEQ, HEADS, SEQ, HS).transpose(0, 2, 1, 3).reshape(TOKENS, HEADS * HS)

def unit_rows(weights):
    weights_f = weights.astype(jnp.float32)
    norms = jnp.sqrt(lax.optimization_barrier(jnp.sum(weights_f * weights_f, axis=1, keepdims=True)) + EPS)
    return (weights_f / norms, norms)

def unit_back(grad_unit, unit, norms):
    row_dot = lax.optimization_barrier(jnp.sum(grad_unit * unit, axis=1, keepdims=True))
    return (grad_unit - unit * row_dot) / norms

def reference(hidden, queries, attn_keys, w_value, w_out, alpha, out_grad):
    unit_v, norm_v = unit_rows(w_value)
    unit_o, norm_o = unit_rows(w_out)
    weight_v = unit_v.astype(jnp.bfloat16)
    weight_o = unit_o.astype(jnp.bfloat16)
    values = contract_last(hidden, weight_v).astype(jnp.bfloat16)
    q_heads = to_heads(queries)
    k_heads = to_heads(attn_keys)
    v_heads = to_heads(values)
    attn = from_heads(lax.map(head_forward, (q_heads, k_heads, v_heads)))
    proj = jnp.dot(attn, weight_o, preferred_element_type=jnp.float32)
    hidden_f = hidden.astype(jnp.float32)
    proj_rs = lax.rsqrt(lax.optimization_barrier(jnp.mean(proj * proj, axis=1, keepdims=True)) + EPS)
    mixed = hidden_f + alpha * (proj * proj_rs - hidden_f)
    mix_rs = lax.rsqrt(lax.optimization_barrier(jnp.mean(mixed * mixed, axis=1, keepdims=True)) + EPS)
    new_hidden = (mixed * mix_rs).astype(jnp.bfloat16)
    grad_out = out_grad.astype(jnp.float32)
    grad_mix = mix_rs * (grad_out - mixed * mix_rs * mix_rs * lax.optimization_barrier(jnp.mean(grad_out * mixed, axis=1, keepdims=True)))
    grad_res = grad_mix * (1.0 - alpha)
    grad_pn = grad_mix * alpha
    grad_proj = proj_rs * (grad_pn - proj * proj_rs * proj_rs * lax.optimization_barrier(jnp.mean(grad_pn * proj, axis=1, keepdims=True)))
    grad_proj_b = grad_proj.astype(jnp.bfloat16)
    grad_attn = contract_last(grad_proj_b, weight_o).astype(jnp.bfloat16)
    gw_o = contract_first(attn, grad_proj_b)
    grad_q, grad_k, grad_v = lax.map(head_backward, (q_heads, k_heads, v_heads, to_heads(grad_attn)))
    grad_values = from_heads(grad_v)
    grad_hidden = (grad_res + jnp.dot(grad_values, weight_v, preferred_element_type=jnp.float32)).astype(jnp.bfloat16)
    gw_v = contract_first(grad_values, hidden)
    grad_w_value = unit_back(gw_v, unit_v, norm_v)
    grad_w_out = unit_back(gw_o, unit_o, norm_o)
    return (new_hidden, grad_hidden, from_heads(grad_q), from_heads(grad_k), grad_w_value, grad_w_out)
```

```python
import jax
import jax.numpy as jnp
from jax import lax
from jax.experimental import pallas as pl
from jax.experimental.pallas import tpu as pltpu
from jax.sharding import PartitionSpec as P

D = 3072
HS = 128


EPS = 1e-06


def contract_last(left, right):
    return lax.dot_general(
        left, right, (((1,), (1,)), ((), ())), preferred_element_type=jnp.float32
    )


def contract_first(left, right):
    return lax.dot_general(
        left, right, (((0,), (0,)), ((), ())), preferred_element_type=jnp.float32
    )


def cost(flops, nbytes):
    return pl.CostEstimate(flops=flops, bytes_accessed=nbytes, transcendentals=0)


def probs_kernel(q_ref, k_ref, probs_ref):
    length = q_ref.shape[0]
    score_scale = q_ref.shape[1] ** (-0.5)
    scores = contract_last(q_ref[...], k_ref[...]) * score_scale
    row_pos = lax.broadcasted_iota(jnp.int32, (length, length), 0)
    col_pos = lax.broadcasted_iota(jnp.int32, (length, length), 1)
    scores = jnp.where(row_pos >= col_pos, scores, -1e30)
    row_peak = jnp.max(scores, axis=1, keepdims=True)
    exp_terms = jnp.exp(scores - row_peak)
    probs_ref[0] = exp_terms * (1.0 / jnp.sum(exp_terms, axis=1, keepdims=True))


def forward_kernel(probs_ref, part_ref, recv_ref, scale_ref, attn_ref, values_ref):
    values = (part_ref[...] + recv_ref[...].astype(jnp.float32)) * scale_ref[...]
    values_b = values.astype(jnp.bfloat16)
    values_ref[...] = values_b
    attn_ref[...] = jnp.dot(
        probs_ref[0].astype(jnp.bfloat16), values_b, preferred_element_type=jnp.float32
    ).astype(jnp.bfloat16)


def backward_kernel(
    probs_ref, q_ref, k_ref, v_ref, part_ref, recv_ref, gq_ref, gk_ref, gv_ref
):
    score_scale = q_ref.shape[1] ** (-0.5)
    grad_head = (part_ref[...] + recv_ref[...].astype(jnp.float32)).astype(jnp.bfloat16)
    probs = probs_ref[0]
    grad_prob = contract_last(grad_head, v_ref[...])
    row_delta = jnp.sum(probs * grad_prob, axis=1, keepdims=True)
    grad_score = (probs * (grad_prob - row_delta)).astype(jnp.bfloat16)
    gv_ref[...] = contract_first(probs.astype(jnp.bfloat16), grad_head).astype(jnp.bfloat16)
    gq_ref[...] = (
        jnp.dot(grad_score, k_ref[...], preferred_element_type=jnp.float32) * score_scale
    ).astype(jnp.bfloat16)
    gk_ref[...] = (contract_first(grad_score, q_ref[...]) * score_scale).astype(jnp.bfloat16)


def head_spec(length):
    return pl.BlockSpec((length, HS), lambda h: (0, h))


def square_spec(length):
    return pl.BlockSpec((1, length, length), lambda h: (h, 0, 0))


def head_probs(queries, keys):
    length, width = queries.shape
    heads = width // HS
    return pl.pallas_call(
        probs_kernel,
        grid=(heads,),
        in_specs=[head_spec(length)] * 2,
        out_specs=square_spec(length),
        out_shape=jax.ShapeDtypeStruct((heads, length, length), jnp.float32),
        cost_estimate=cost(heads * 30 * HS * length * length, 4 * heads * length * length),
    )(queries, keys)


def attend(probs, part, recv, scale):
    length, width = part.shape
    heads = width // HS
    one = head_spec(length)
    shape = jax.ShapeDtypeStruct((length, width), jnp.bfloat16)
    return pl.pallas_call(
        forward_kernel,
        grid=(heads,),
        in_specs=[square_spec(length), one, one, pl.BlockSpec((1, HS), lambda h: (0, h))],
        out_specs=[one, one],
        out_shape=[shape, shape],
        cost_estimate=cost(heads * 4 * HS * length * length, 6 * heads * length * length),
    )(probs, part, recv, scale)


def attend_backward(probs, queries, keys, values, part, recv):
    length, width = part.shape
    heads = width // HS
    one = head_spec(length)
    shape = jax.ShapeDtypeStruct((length, width), jnp.bfloat16)
    return pl.pallas_call(
        backward_kernel,
        grid=(heads,),
        in_specs=[square_spec(length)] + [one] * 5,
        out_specs=[one] * 3,
        out_shape=[shape] * 3,
        cost_estimate=cost(heads * 30 * HS * length * length, 6 * heads * length * length),
    )(probs, queries, keys, values, part, recv)


def shards(hidden, queries, attn_keys, w_value, w_out, alpha, out_grad):
    groups = lax.axis_size("grp")
    assert groups == 2
    me = lax.axis_index("grp")
    swap = [(0, 1), (1, 0)]

    def exchange(block):
        return lax.ppermute(block, "grp", swap)

    def mine_and_other(weight):
        rows = weight.shape[0] // groups
        return (
            lax.dynamic_slice_in_dim(weight, me * rows, rows, 0),
            lax.dynamic_slice_in_dim(weight, (1 - me) * rows, rows, 0),
        )

    def in_order(mine, other):
        return jnp.concatenate(
            (jnp.where(me == 0, mine, other), jnp.where(me == 0, other, mine)), axis=1
        )

    raw_v = lax.all_gather(w_value, "fsdp", axis=0, tiled=True)
    value_rows = w_value.astype(jnp.float32)
    out_rows = w_out.astype(jnp.float32)
    own_sums = jnp.stack(
        (jnp.sum(value_rows * value_rows, axis=1), jnp.sum(out_rows * out_rows, axis=1))
    )
    own_sums = own_sums + exchange(own_sums)
    norms = jnp.sqrt(own_sums + EPS)
    norm_v = norms[0][:, None]
    norm_o = norms[1][:, None]
    unit_v = value_rows / norm_v
    unit_o = out_rows / norm_o
    weight_o = lax.all_gather(unit_o.astype(jnp.bfloat16), "fsdp", axis=0, tiled=True)
    all_norm_v = lax.all_gather(norms[0], "fsdp", axis=0, tiled=True)
    probs = head_probs(queries, attn_keys)

    raw_mine, raw_other = mine_and_other(raw_v)
    value_recv = exchange(contract_last(hidden, raw_other).astype(jnp.bfloat16))
    value_part = contract_last(hidden, raw_mine)
    width = queries.shape[1]
    scale = 1.0 / lax.dynamic_slice_in_dim(all_norm_v, me * width, width, 0)
    attn_mine, values = attend(probs, value_part, value_recv, scale[None, :])
    weight_v = (raw_v.astype(jnp.float32) / all_norm_v[:, None]).astype(jnp.bfloat16)
    attn_all = in_order(attn_mine, exchange(attn_mine))
    proj = jnp.dot(attn_all, weight_o, preferred_element_type=jnp.float32)
    hidden_f = hidden.astype(jnp.float32)
    keep_rate = 1.0 - alpha
    grad_out = out_grad.astype(jnp.float32)
    moments = jnp.stack(
        (
            jnp.sum(proj * proj, axis=1),
            jnp.sum(keep_rate * keep_rate * hidden_f * hidden_f, axis=1),
            jnp.sum(keep_rate * alpha * hidden_f * proj, axis=1),
            jnp.sum(alpha * alpha * proj * proj, axis=1),
            jnp.sum(grad_out * keep_rate * hidden_f, axis=1),
            jnp.sum(grad_out * alpha * proj, axis=1),
        )
    )
    moments = moments + exchange(moments)
    proj_rs = lax.rsqrt(moments[0] / D + EPS)[:, None]
    cross_sum = moments[2][:, None]
    alpha_sum = moments[3][:, None]
    mix_mean = (moments[1][:, None] + 2.0 * proj_rs * cross_sum + proj_rs * proj_rs * alpha_sum) / D
    mix_rs = lax.rsqrt(mix_mean + EPS)
    mixed = hidden_f + alpha * (proj * proj_rs - hidden_f)
    new_hidden = (mixed * mix_rs).astype(jnp.bfloat16)
    grad_mean = (moments[4][:, None] + proj_rs * moments[5][:, None]) / D
    grad_mix = mix_rs * (grad_out - mixed * mix_rs * mix_rs * grad_mean)
    grad_pn = grad_mix * alpha
    proj_mean = (
        mix_rs * moments[5][:, None]
        - mix_rs * mix_rs * mix_rs * grad_mean * (cross_sum + proj_rs * alpha_sum)
    ) / D
    grad_res = grad_mix * keep_rate
    grad_proj = proj_rs * (grad_pn - proj * proj_rs * proj_rs * proj_mean)
    grad_proj_b = grad_proj.astype(jnp.bfloat16)
    out_mine, out_other = mine_and_other(weight_o)
    grad_recv = exchange(contract_last(grad_proj_b, out_other).astype(jnp.bfloat16))
    grad_part = contract_last(grad_proj_b, out_mine)
    gw_o_own = lax.psum_scatter(
        contract_first(attn_all, grad_proj_b).astype(jnp.bfloat16),
        "fsdp",
        scatter_dimension=0,
        tiled=True,
    ).astype(jnp.float32)
    grad_q, grad_k, grad_v = attend_backward(
        probs, queries, attn_keys, values, grad_part, grad_recv
    )
    grad_values = in_order(grad_v, exchange(grad_v))
    gw_v_own = lax.psum_scatter(
        contract_first(grad_values, hidden).astype(jnp.bfloat16),
        "fsdp",
        scatter_dimension=0,
        tiled=True,
    ).astype(jnp.float32)
    grad_hidden = (
        grad_res + jnp.dot(grad_values, weight_v, preferred_element_type=jnp.float32)
    ).astype(jnp.bfloat16)
    dot_o = jnp.sum(gw_o_own * unit_o, axis=1, keepdims=True)
    dot_o = dot_o + exchange(dot_o)
    grad_w_out = (gw_o_own - unit_o * dot_o) / norm_o
    dot_v = jnp.sum(gw_v_own * unit_v, axis=1, keepdims=True)
    dot_v = dot_v + exchange(dot_v)
    grad_w_value = (gw_v_own - unit_v * dot_v) / norm_v
    return (new_hidden, grad_hidden, grad_q, grad_k, grad_w_value, grad_w_out)


def solution(mesh):
    placed = (
        P("fsdp", "grp"),
        P("fsdp", "grp"),
        P("fsdp", "grp"),
        P("fsdp", "grp"),
        P("fsdp", "grp"),
        P("grp"),
        P("fsdp", "grp"),
    )
    return jax.shard_map(
        shards,
        mesh=mesh,
        in_specs=placed,
        out_specs=(
            P("fsdp", "grp"),
            P("fsdp", "grp"),
            P("fsdp", "grp"),
            P("fsdp", "grp"),
            P("fsdp", "grp"),
            P("fsdp", "grp"),
        ),
        check_vma=False,
    )
```
